16 devices in a mesh: dp: 4 (over y, z, core), tp: 4 (over x).
Axes of the slice: x: 4, y: 2, z: 1, core: 2. Of those that a mesh axis runs over, the one named last changes fastest.
The devices are a block of a 4x4x8 slice.
Arguments:
- x: bfloat16 [4096, 7168], P(('dp', 'tp')), parts along dimension 0
- gain_a: bfloat16 [7168], replicated
- wq: bfloat16 [7168, 7168], P(None, 'tp')
- wk: bfloat16 [7168, 1024], P(None, 'tp')
- wv: bfloat16 [7168, 1024], P(None, 'tp')
- wo: bfloat16 [7168, 7168], P('tp')
- gain_m: bfloat16 [7168], replicated
- w_gate: bfloat16 [7168, 20480], P(None, 'tp')
- w_up: bfloat16 [7168, 20480], P(None, 'tp')
- w_down: bfloat16 [20480, 7168], P('tp')
Outputs:
- output: bfloat16 [4096, 7168], P(('dp', 'tp')), parts along dimension 0
There are 4 independent parts. The reference program is written for one: setup_inputs(seed, part) draws one part's arguments, and reference() takes and returns one part's arrays. A program takes and returns all parts, laid end to end along the dimension named above; an argument that names none is the same for every part.
All inputs are finite; a program needn't handle non-finite values.
Results may differ from the reference program's by a relative error of at most 0.017.
Values are sent between devices in bfloat16 or wider.
A program may use at most 768 MiB of HBM per device.

```python
import jax
import jax.numpy as jnp
from jax import lax

ROWS = 1024
D = 7168
HEADS = 56
KV_HEADS = 8
HEAD = 128
FF = 20480
THETA = 10000


def setup_inputs(seed: int = 0, part: int = 0) -> dict:
    kx, kn, kq, kk, kv, ko, km, kg, ku, kd = jax.random.split(jax.random.key(seed), 10)

    def weights(key, rows, columns):
        return jax.random.normal(key, (rows, columns), jnp.float32) * rows**-0.5

    drawn = {
        "x": jax.random.normal(jax.random.fold_in(kx, part), (ROWS, D), jnp.float32),
        "gain_a": 1 + 0.1 * jax.random.normal(kn, (D,), jnp.float32),
        "wq": 2 * weights(kq, D, HEADS * HEAD),
        "wk": 2 * weights(kk, D, KV_HEADS * HEAD),
        "wv": 4 * weights(kv, D, KV_HEADS * HEAD),
        "wo": weights(ko, HEADS * HEAD, D),
        "gain_m": 1 + 0.1 * jax.random.normal(km, (D,), jnp.float32),
        "w_gate": weights(kg, D, FF),
        "w_up": weights(ku, D, FF),
        "w_down": 2 * weights(kd, FF, D),
    }
    return {k: v.astype(jnp.bfloat16) for k, v in drawn.items()}


def normed(x, gain):
    wide = x.astype(jnp.float32)
    scale = lax.rsqrt(jnp.mean(wide * wide, -1, keepdims=True) + 1e-6)
    return (wide * scale * gain.astype(jnp.float32)).astype(jnp.bfloat16)


def turned(t, place, theta):
    half = t.shape[-1] // 2
    angle = place.astype(jnp.float32)[:, None] * theta ** (-jnp.arange(half, dtype=jnp.float32) / half)
    cos, sin = jnp.cos(angle)[:, None], jnp.sin(angle)[:, None]
    a, b = t[..., :half].astype(jnp.float32), t[..., half:].astype(jnp.float32)
    return jnp.concatenate([a * cos - b * sin, b * cos + a * sin], -1).astype(jnp.bfloat16)


def matmul(a, w):
    return jnp.dot(a, w, preferred_element_type=jnp.float32).astype(jnp.bfloat16)


def einsum(form, a, b):
    return jnp.einsum(form, a.astype(jnp.float32), b.astype(jnp.float32))


def attention(q, k, v):
    scores = einsum("tgsd,ugd->gstu", q, k) * q.shape[-1] ** -0.5
    token = jnp.arange(q.shape[0])
    scores = jnp.where(token[:, None] >= token, scores, -jnp.inf)
    weights = jax.nn.softmax(scores, -1).astype(jnp.bfloat16)
    return einsum("gstu,ugd->tgsd", weights, v).astype(jnp.bfloat16)


def reference(x, gain_a, wq, wk, wv, wo, gain_m, w_gate, w_up, w_down):
    a, place = normed(x, gain_a), jnp.arange(ROWS)
    q = turned(matmul(a, wq).reshape(ROWS, HEADS, HEAD), place, THETA).reshape(ROWS, KV_HEADS, -1, HEAD)
    k = turned(matmul(a, wk).reshape(ROWS, KV_HEADS, HEAD), place, THETA)
    v = matmul(a, wv).reshape(ROWS, KV_HEADS, HEAD)
    seen = attention(q, k, v).reshape(ROWS, HEADS * HEAD)
    h = (x.astype(jnp.float32) + jnp.dot(seen, wo, preferred_element_type=jnp.float32)).astype(jnp.bfloat16)
    b = normed(h, gain_m)
    gate = jnp.dot(b, w_gate, preferred_element_type=jnp.float32)
    up = jnp.dot(b, w_up, preferred_element_type=jnp.float32)
    hidden = (jax.nn.silu(gate) * up).astype(jnp.bfloat16)
    return (h.astype(jnp.float32) + jnp.dot(hidden, w_down, preferred_element_type=jnp.float32)).astype(jnp.bfloat16)
```

```python
import functools

import jax
import jax.numpy as jnp
from jax import lax
from jax.experimental import pallas as pl
from jax.experimental.pallas import tpu as pltpu
from jax.sharding import PartitionSpec as P

HEAD = 128
THETA = 10000
NEG = -1e30
HIDDEN = 2 * NEG
LOG2E = 1.4426950408889634
BF16, F32 = jnp.bfloat16, jnp.float32


def _dot(a, b, ca, cb):
    return lax.dot_general(a, b, (((ca,), (cb,)), ((), ())), preferred_element_type=F32)


def _turn(t, cos, sin):
    return (t * cos + pltpu.roll(t, HEAD // 2, 1) * sin).astype(BF16)


def _attend_kernel(at_ref, q_ref, ka_ref, kb_ref, va_ref, vb_ref, cosq_ref, sinq_ref, cos_ref, sin_ref, o_ref,
                   k_s, v_s, q_s, top_s, mix_s, *, block, heads, first):
    iq = pl.program_id(1)
    blocks = k_s.shape[0]
    e = HEAD**-0.5 * LOG2E

    @pl.when(iq == 0)
    def _():
        ones = jnp.ones((8, block), BF16)
        for j in range(blocks):
            rows = pl.ds(j * block, block)
            if j < blocks - 1:
                k, v = ka_ref[rows, :], va_ref[rows, :]
            else:
                k, v = kb_ref[...], vb_ref[...]
            k_s[j] = _turn(k.astype(F32), cos_ref[rows, :], sin_ref[rows, :])
            v_s[j, :HEAD, :] = v.T
            v_s[j, HEAD:, :] = ones

    for h in range(heads):
        q_s[h * block : (h + 1) * block, :] = _turn(q_ref[:, h * HEAD : (h + 1) * HEAD].astype(F32), cosq_ref[...], sinq_ref[...])
    top_s[...] = jnp.full(top_s.shape, NEG, F32)
    mix_s[...] = jnp.zeros(mix_s.shape, F32)
    mine = first + iq
    strips = [pl.ds(h * block, block) for h in range(heads)]

    def step(j, masked):
        keys, values = k_s[j], v_s[j]
        scores = [_dot(keys, q_s[at, :], 1, 1) for at in strips]
        weights, keeps = [], []
        if masked:
            seen = lax.broadcasted_iota(jnp.int32, (block, block), 1) >= lax.broadcasted_iota(jnp.int32, (block, block), 0)
        for at, s in zip(strips, scores):
            if masked:
                s = jnp.where(seen, s, HIDDEN)
            old = top_s[:, at]
            top = jnp.maximum(old, s.max(axis=0, keepdims=True))
            top_s[:, at] = top
            weights.append(jnp.exp2((s - top) * e).astype(BF16))
            keeps.append(jnp.exp2((old - top) * e))
        for at, p, keep in zip(strips, weights, keeps):
            mix_s[:, at] = mix_s[:, at] * keep + _dot(values, p, 1, 0)

    place = at_ref[mine]

    def earlier(j, _):
        @pl.when(at_ref[j] < place)
        def _():
            step(j, False)

    lax.fori_loop(0, blocks, earlier, None)
    step(mine, True)
    for h, at in enumerate(strips):
        o_ref[:, h * HEAD : (h + 1) * HEAD] = (mix_s[:HEAD, at] * (1 / mix_s[HEAD : HEAD + 1, at])).T.astype(BF16)


def attend(at, q, ka, kb, va, vb, cos, sin, first):
    block, kv = kb.shape[0], kb.shape[1] // HEAD
    blocks = ka.shape[0] // block + 1
    heads = q.shape[1] // HEAD // kv
    wide = heads * HEAD
    here = lambda g, i, _: (i + first, 0)
    whole = lambda g, i, _: (0, 0)
    some = lambda g, i, _: (0, g)
    return pl.pallas_call(
        functools.partial(_attend_kernel, block=block, heads=heads, first=first),
        grid_spec=pltpu.PrefetchScalarGridSpec(
            num_scalar_prefetch=1,
            grid=(kv, q.shape[0] // block),
            in_specs=[
                pl.BlockSpec((block, wide), lambda g, i, _: (i, g)),
                pl.BlockSpec((ka.shape[0], HEAD), some),
                pl.BlockSpec((block, HEAD), some),
                pl.BlockSpec((ka.shape[0], HEAD), some),
                pl.BlockSpec((block, HEAD), some),
                pl.BlockSpec((block, HEAD), here),
                pl.BlockSpec((block, HEAD), here),
                pl.BlockSpec((blocks * block, HEAD), whole),
                pl.BlockSpec((blocks * block, HEAD), whole),
            ],
            out_specs=pl.BlockSpec((block, wide), lambda g, i, _: (i, g)),
            scratch_shapes=[
                pltpu.VMEM((blocks, block, HEAD), BF16),
                pltpu.VMEM((blocks, HEAD + 8, block), BF16),
                pltpu.VMEM((heads * block, HEAD), BF16),
                pltpu.VMEM((1, heads * block), F32),
                pltpu.VMEM((HEAD + 8, heads * block), F32),
            ],
        ),
        out_shape=jax.ShapeDtypeStruct(q.shape, BF16),
        compiler_params=pltpu.CompilerParams(dimension_semantics=("arbitrary", "arbitrary"), vmem_limit_bytes=40 * 2**20),
        cost_estimate=pl.CostEstimate(flops=4 * q.size * blocks * block * 5 // 8, transcendentals=q.size // HEAD * blocks * block,
                                      bytes_accessed=4 * q.size + 4 * blocks * block * kv * HEAD),
    )(at, q, ka, kb, va, vb, cos, sin, cos, sin)


def _norm_kernel(x_ref, gain_ref, b_ref):
    wide = x_ref[...].astype(F32)
    scale = lax.rsqrt(jnp.mean(wide * wide, -1, keepdims=True) + 1e-6)
    b_ref[...] = (wide * scale * gain_ref[...].astype(F32)).astype(BF16)


def normed(x, gain):
    rows, d = x.shape
    step = 32
    return pl.pallas_call(
        _norm_kernel,
        grid=(rows // step,),
        in_specs=[pl.BlockSpec((step, d), lambda i: (i, 0)), pl.BlockSpec((1, d), lambda i: (0, 0))],
        out_specs=pl.BlockSpec((step, d), lambda i: (i, 0)),
        out_shape=jax.ShapeDtypeStruct(x.shape, BF16),
        compiler_params=pltpu.CompilerParams(vmem_limit_bytes=16 * 2**20),
        cost_estimate=pl.CostEstimate(flops=4 * x.size * 400, transcendentals=rows, bytes_accessed=4 * x.size),
    )(x, gain[None])


GROUP, TILE = 512, 256
LAG = 4
MESH = pl.DeviceIdType.MESH


def _tail_kernel(n, seen, far, x, gain, wo, wg, wu, wd, y, hid_s, b_s, h_s, w_s, via_s, near_s, own_s, part_s, far_s, send_s, ss_s,
                 load_sem, x_sem, w_sem, far_sem, send_sem, via_sem, near_sem, ag_send, ag_recv):
    me = lax.axis_index("tp")
    right, left = {"tp": lax.rem(me + 1, n)}, {"tp": lax.rem(me + n - 1, n)}
    p_rows = h_s.shape[1]
    half = p_rows // 2
    all_rows, d = b_s.shape[1], b_s.shape[2]
    groups = d // GROUP
    wo_k, ff = wo.shape[0], wd.shape[0]
    rows_here = far.shape[0]
    tiles = ff // 128
    part = all_rows // 2

    def columns(i, size):
        return pl.ds(pl.multiple_of(i * size, size), size)

    barrier = pltpu.get_barrier_semaphore()
    for neighbour in (left, right):
        pl.semaphore_signal(barrier, inc=1, device_id=neighbour, device_id_type=MESH)

    def loads(p):
        at = [far.at[pl.ds(p * p_rows, p_rows), :]]
        at += [seen.at[pl.ds(i * rows_here + p * p_rows, p_rows), :] for i in (1, 2, 0)]
        return [pltpu.make_async_copy(src, hid_s.at[pl.ds(i * p_rows, p_rows), pl.ds(p * wo_k, wo_k)], load_sem.at[p, i])
                for i, src in enumerate(at)]

    def x_load(p):
        return pltpu.make_async_copy(x.at[pl.ds(p * p_rows, p_rows), :], h_s.at[p], x_sem.at[p])

    def y_store(p):
        return pltpu.make_async_copy(h_s.at[p], y.at[pl.ds(p * p_rows, p_rows), :], x_sem.at[p])

    def wo_load(g, slot):
        return [pltpu.make_async_copy(wo.at[:, columns(g * (GROUP // TILE) + s, TILE)], w_s.at[slot, pl.ds(s * wo_k, wo_k), :],
                                      w_sem.at[slot, s]) for s in range(GROUP // TILE)]

    def gu_load(k, slot):
        return [pltpu.make_async_copy(w.at[:, columns(k, 128)], w_s.at[slot, :, pl.ds(i * 128, 128)], w_sem.at[slot, i])
                for i, w in enumerate((wg, wu))]

    def wd_load(m, slot):
        return [pltpu.make_async_copy(wd.at[:, columns(m, TILE)], w_s.at[slot, pl.ds(0, ff), :], w_sem.at[slot, 0])]

    def start(copies):
        for c in copies:
            c.start()

    def wait(copies):
        for c in copies:
            c.wait()

    def remote(src, dst, s_sem, r_sem, to):
        return pltpu.make_async_remote_copy(src_ref=src, dst_ref=dst, send_sem=s_sem, recv_sem=r_sem, device_id=to, device_id_type=MESH)

    def far_copies(p, g):
        return [remote(far_s.at[g, pl.ds(i * half, half), :], via_s.at[p, g, pl.ds(i * half, half), :], far_sem.at[g, i],
                       via_sem.at[p, g, i], to) for i, to in enumerate((right, left))]

    def near_copies(p, g):
        return [remote(send_s.at[g, i], near_s.at[p, i, g], send_sem.at[g, i], near_sem.at[p, g, i], to)
                for i, to in enumerate((right, left))]

    def keep(g, s, i, acc):
        cols = pl.ds(s * TILE, TILE)
        first, second = acc[:p_rows], acc[p_rows:]
        if i == 0:
            far_s[g, :, cols] = first.astype(BF16)
            part_s[g, pl.ds(p_rows, p_rows), cols] = second
        else:
            part_s[g, pl.ds(0, p_rows), cols] = first
            own_s[g, :, cols] = second

    def pass_on(p, g):
        for c in far_copies(p, g):
            c.wait_recv()
        send_s[g, 0, pl.ds(0, half), :] = (part_s[g, pl.ds(0, half), :] + via_s[p, g, pl.ds(0, half), :].astype(F32)).astype(BF16)
        send_s[g, 0, pl.ds(half, half), :] = part_s[g, pl.ds(half, half), :].astype(BF16)
        send_s[g, 1, pl.ds(0, half), :] = part_s[g, pl.ds(2 * half, half), :].astype(BF16)
        send_s[g, 1, pl.ds(half, half), :] = (part_s[g, pl.ds(3 * half, half), :] + via_s[p, g, pl.ds(half, half), :].astype(F32)).astype(BF16)
        start(near_copies(p, g))

    def add_up(p, g, norm):
        for c in near_copies(p, g):
            c.wait_recv()
        cols = columns(g, GROUP)
        total = own_s[g] + near_s[p, 0, g].astype(F32) + near_s[p, 1, g].astype(F32)
        h = (h_s[p, :, cols].astype(F32) + total).astype(BF16)
        h_s[p, :, cols] = h
        if norm:
            h = h.astype(F32)
            h = h * h
            ss_s[...] += sum(h[:, i * 128 : (i + 1) * 128] for i in range(GROUP // 128))

    def sent(p):
        def one(g, _):
            for c in far_copies(p, g) + near_copies(p, g):
                c.wait_send()
        lax.fori_loop(0, groups, one, None)

    def scale_rows(p):
        scale = lax.rsqrt(jnp.sum(ss_s[...], -1, keepdims=True) / d + 1e-6)

        def one(g, _):
            cols = columns(g, GROUP)
            b_s[p, pl.ds(3 * p_rows, p_rows), cols] = (h_s[p, :, cols].astype(F32) * scale * gain[:, cols]).astype(BF16)

        lax.fori_loop(0, groups, one, None)
        ss_s[...] = jnp.zeros(ss_s.shape, F32)

    def rows_of(p, block, i):
        return b_s.at[p, pl.ds(block * p_rows + i * half, half), :]

    def own_copies(p):
        return [remote(rows_of(p, 3, i), rows_of(p, block, i), ag_send.at[p, block, i], ag_recv.at[p, block, i], to)
                for block, i, to in ((1, 0, right), (2, 1, left), (1, 1, right), (2, 0, left))]

    def forwards(p):
        return [remote(rows_of(p, block, i), rows_of(p, 0, i), ag_send.at[p, 0, i], ag_recv.at[p, 0, i], to)
                for block, i, to in ((1, 0, right), (2, 1, left))]

    def forward(p):
        for c in own_copies(p)[:2]:
            c.wait_recv()
        start(forwards(p))

    def gathered(p):
        for c in own_copies(p)[2:] + forwards(p):
            c.wait_recv()

    def out_project(p):
        def one(g, _):
            slot = lax.rem(g, 2)

            @pl.when(g + 1 < groups)
            def _():
                start(wo_load(g + 1, 1 - slot))

            wait(wo_load(g, slot))
            for s in range(GROUP // TILE):
                for i in range(2):
                    keep(g, s, i, jnp.dot(hid_s[pl.ds(i * part, part), pl.ds(p * wo_k, wo_k)], w_s[slot, pl.ds(s * wo_k, wo_k), :],
                                          preferred_element_type=F32))
            start(far_copies(p, g))
            if p == 0:
                @pl.when(g >= LAG)
                def _():
                    pass_on(p, g - LAG)

        lax.fori_loop(0, groups, one, None)

    def gate_up(p, beside):
        def one(k, _):
            slot = lax.rem(k, 2)

            @pl.when(k + 1 < tiles)
            def _():
                start(gu_load(k + 1, 1 - slot))

            @pl.when(k + 1 == tiles)
            def _():
                start(wd_load(0, 0))

            wait(gu_load(k, slot))
            for i in range(2):
                both = jnp.dot(b_s[p, pl.ds(i * part, part), :], w_s[slot], preferred_element_type=F32)
                gate, up = both[:, :128], both[:, 128:]
                hid_s[pl.ds(i * part, part), columns(k, 128)] = (gate * lax.logistic(gate) * up).astype(BF16)
            beside(k)

        lax.fori_loop(0, tiles, one, None)

    def down(p):
        steps = GROUP // TILE

        def one(g, _):
            for s in range(steps):
                m = g * steps + s
                if s + 1 < steps:
                    start(wd_load(m + 1, (s + 1) % 2))
                else:
                    @pl.when(g + 1 < groups)
                    def _():
                        start(wd_load(m + 1, (s + 1) % 2))

                    if p == 0:
                        @pl.when(g + 1 == groups)
                        def _():
                            start(gu_load(0, 0))

                wait(wd_load(m, s % 2))
                for i in range(2):
                    keep(g, s, i, jnp.dot(hid_s[pl.ds(i * part, part), :], w_s[s % 2, pl.ds(0, ff), :], preferred_element_type=F32))
            start(far_copies(p, g))
            if p == 1:
                @pl.when(g >= LAG)
                def _():
                    pass_on(p, g - LAG)

        lax.fori_loop(0, groups, one, None)

    def each(lo, hi, do):
        lax.fori_loop(lo, hi, lambda g, _: do(g), None)

    start(wo_load(0, 0))
    for p in range(2):
        start(loads(p))
        x_load(p).start()
    ss_s[...] = jnp.zeros(ss_s.shape, F32)
    pl.semaphore_wait(barrier, 2)

    wait(loads(0))
    out_project(0)
    start(wo_load(0, 0))
    each(groups - LAG, groups, lambda g: pass_on(0, g))
    x_load(0).wait()
    each(0, groups, lambda g: add_up(0, g, True))
    sent(0)
    scale_rows(0)
    start(own_copies(0))
    forward(0)
    wait(loads(1))
    out_project(1)
    start(gu_load(0, 0))
    x_load(1).wait()
    gathered(0)

    def beside_first(k):
        @pl.when(k < groups)
        def _():
            pass_on(1, k)

        @pl.when((k >= groups) & (k < 2 * groups))
        def _():
            add_up(1, k - groups, True)

        @pl.when(k == 2 * groups)
        def _():
            sent(1)
            scale_rows(1)
            start(own_copies(1))

        @pl.when(k == tiles - 2)
        def _():
            forward(1)

    gate_up(0, beside_first)
    down(0)
    gathered(1)

    def beside_second(k):
        @pl.when(k < groups)
        def _():
            pass_on(0, k)

        @pl.when((k >= groups) & (k < 2 * groups))
        def _():
            add_up(0, k - groups, False)

    gate_up(1, beside_second)
    sent(0)
    y_store(0).start()
    down(1)
    each(groups - LAG, groups, lambda g: pass_on(1, g))
    each(0, groups, lambda g: add_up(1, g, False))
    y_store(1).start()
    sent(1)
    for p in range(2):
        for c in own_copies(p) + forwards(p):
            c.wait_send()
        y_store(p).wait()


def tail(n, seen, far, x, gain, wo, wg, wu, wd):
    rows, d = x.shape
    p_rows = rows // 2
    groups, ff = d // GROUP, wd.shape[0]
    dma = pltpu.SemaphoreType.DMA
    hbm = pl.BlockSpec(memory_space=pl.ANY)
    return pl.pallas_call(
        functools.partial(_tail_kernel, n),
        in_specs=[hbm, hbm, hbm, pl.BlockSpec(memory_space=pltpu.VMEM), hbm, hbm, hbm, hbm],
        out_specs=hbm,
        out_shape=jax.ShapeDtypeStruct(x.shape, BF16),
        scratch_shapes=[
            pltpu.VMEM((n * p_rows, ff), BF16),
            pltpu.VMEM((2, n * p_rows, d), BF16),
            pltpu.VMEM((2, p_rows, d), BF16),
            pltpu.VMEM((2, d, TILE), BF16),
            pltpu.VMEM((2, groups, p_rows, GROUP), BF16),
            pltpu.VMEM((2, 2, groups, p_rows, GROUP), BF16),
            pltpu.VMEM((groups, p_rows, GROUP), F32),
            pltpu.VMEM((groups, 2 * p_rows, GROUP), F32),
            pltpu.VMEM((groups, p_rows, GROUP), BF16),
            pltpu.VMEM((groups, 2, p_rows, GROUP), BF16),
            pltpu.VMEM((p_rows, 128), F32),
            dma((2, n)), dma((2,)), dma((2, 2)), dma((groups, 2)), dma((groups, 2)), dma((2, groups, 2)), dma((2, groups, 2)),
            dma((2, 3, 2)), dma((2, 3, 2)),
        ],
        compiler_params=pltpu.CompilerParams(collective_id=0, has_side_effects=True, vmem_limit_bytes=67043328),
        cost_estimate=pl.CostEstimate(flops=2 * n * rows * d * (wo.shape[0] + 3 * ff), transcendentals=n * rows * ff,
                                      bytes_accessed=2 * d * (wo.shape[0] + 6 * ff)),
    )(seen, far, x, gain.astype(F32)[None], wo, wg, wu, wd)


def solution(mesh):
    n = mesh.shape["tp"]
    to_right = [(i, (i + 1) % n) for i in range(n)]
    to_left = [(i, (i - 1) % n) for i in range(n)]

    def right(t):
        return lax.ppermute(t, "tp", to_right)

    def left(t):
        return lax.ppermute(t, "tp", to_left)

    def halves(t):
        return t[: t.shape[0] // 2], t[t.shape[0] // 2 :]

    def gathered(t):
        from_left, from_right = right(t), left(t)
        return from_left, from_right, right(halves(from_left)[0]), left(halves(from_right)[1])

    def mm(a, w):
        return jnp.dot(a, w, preferred_element_type=F32)

    def step(x, gain_a, wq, wk, wv, wo, gain_m, w_gate, w_up, w_down):
        rows = x.shape[0]
        me = lax.axis_index("tp")
        at = jnp.stack([me, (me + n - 1) % n, (me + 1) % n, (me + 2) % n]).astype(jnp.int32)
        half = HEAD // 2
        place = (at[:, None] * rows + jnp.arange(rows)[None]).reshape(-1).astype(F32)
        angle = place[:, None] * THETA ** (-jnp.arange(half, dtype=F32) / half)
        cos, sin = jnp.cos(angle), jnp.sin(angle)
        cos, sin = jnp.concatenate([cos, cos], -1), jnp.concatenate([-sin, sin], -1)

        a = normed(x, gain_a)
        from_left, from_right, o0, o1 = gathered(a)
        weights = (wq, wk, wv)
        own = [mm(a, w).astype(BF16) for w in weights]
        near = jnp.concatenate([from_left, from_right])
        near = [mm(near, w).astype(BF16) for w in weights]
        far = jnp.concatenate([o0, o1])
        qo, ko, vo = [mm(far, w).astype(BF16) for w in weights]
        q, k, v = [jnp.concatenate(pair) for pair in zip(own, near)]
        seen_far = attend(at, qo, k, ko, v, vo, cos, sin, n - 1)
        seen = attend(at, q, k, ko, v, vo, cos, sin, 0)

        return tail(n, seen, seen_far, x, gain_m, wo, w_gate, w_up, w_down)

    tokens, columns, rows_of = P(("dp", "tp"), None), P(None, "tp"), P("tp", None)
    return jax.shard_map(
        step,
        mesh=mesh,
        in_specs=(tokens, P(None), columns, columns, columns, rows_of, P(None), columns, columns, rows_of),
        out_specs=tokens,
        check_vma=False,
    )
```

```python
import functools

import jax
import jax.numpy as jnp
import numpy as np
from jax import lax
from jax.experimental import pallas as pl
from jax.experimental.pallas import tpu as pltpu
from jax.sharding import PartitionSpec as P

HEAD = 128
THETA = 10000
NEG = -1e30
HIDDEN = 2 * NEG
LOG2E = 1.4426950408889634
BF16, F32 = jnp.bfloat16, jnp.float32


MESH = pl.DeviceIdType.MESH
TILE = 256


def _columns(i, size):
    return pl.ds(pl.multiple_of(i * size, size), size)


def _neighbours(n):
    me = lax.axis_index("tp")
    return {"tp": lax.rem(me + 1, n)}, {"tp": lax.rem(me + n - 1, n)}


def _greet(neighbours):
    barrier = pltpu.get_barrier_semaphore()
    for neighbour in neighbours:
        pl.semaphore_signal(barrier, inc=1, device_id=neighbour, device_id_type=MESH)


def _greeted():
    pl.semaphore_wait(pltpu.get_barrier_semaphore(), 2)


def _remote(src, dst, s_sem, r_sem, to):
    return pltpu.make_async_remote_copy(src_ref=src, dst_ref=dst, send_sem=s_sem, recv_sem=r_sem, device_id=to, device_id_type=MESH)


def _start(copies):
    for c in copies:
        c.start()


def _wait(copies):
    for c in copies:
        c.wait()


def _each(lo, hi, do):
    lax.fori_loop(lo, hi, lambda i, _: do(i), None)


def _dot(a, b, ca=1, cb=0):
    return lax.dot_general(a, b, (((ca,), (cb,)), ((), ())), preferred_element_type=F32)


def _head_kernel(n, heads, kv, x, gain, table, wq, wk, wv, out, b_s, w_s, q_s, k_s, v_s, cos_s, sin_s, top_s, mix_s, o_s,
                 x_sem, w_sem, o_sem, t_sem, ag_send, ag_recv):
    right, left = _neighbours(n)
    me = lax.axis_index("tp")
    rows, d = x.shape
    half, group = rows // 2, heads // kv
    q_tiles = heads * HEAD // TILE
    e = HEAD**-0.5 * LOG2E
    own, far = 0, n - 1

    def place(block):
        step = jnp.where(block == 0, 0, jnp.where(block == 1, n - 1, block - 1))
        return lax.rem(me + step, n)

    _greet((left, right))
    x_loads = [pltpu.make_async_copy(x.at[pl.ds(i * half, half), :], b_s.at[own, pl.ds(i * half, half), :], x_sem.at[i]) for i in range(2)]
    _start(x_loads)

    def table_load(block):
        return pltpu.make_async_copy(table.at[place(block)], cos_s.at[block], t_sem.at[block])


    def q_load(j):
        return pltpu.make_async_copy(wq.at[:, _columns(j, TILE)], w_s.at[lax.rem(j, 3)], w_sem.at[lax.rem(j, 3)])

    def kv_load(i):
        slot = (q_tiles + i) % 3
        return pltpu.make_async_copy((wk, wv)[i], w_s.at[slot], w_sem.at[slot])

    for block in range(n):
        table_load(block).start()
    q_load(0).start()
    q_load(1).start()

    strip = 16

    def norm(i):
        at = pl.ds(pl.multiple_of(i * strip, strip), strip)
        wide = b_s[own, at, :].astype(F32)
        scale = lax.rsqrt(jnp.mean(wide * wide, -1, keepdims=True) + 1e-6)
        b_s[own, at, :] = (wide * scale * gain[0:1, :]).astype(BF16)

    def part(block, i):
        return b_s.at[block, pl.ds(i * half, half), :]

    own_copies = [_remote(part(own, i), part(block, i), ag_send.at[block, i], ag_recv.at[block, i], to)
                  for block, i, to in ((1, 0, right), (2, 1, left), (1, 1, right), (2, 0, left))]
    forwards = [_remote(part(block, i), part(far, i), ag_send.at[far, i], ag_recv.at[far, i], to)
                for block, i, to in ((1, 0, right), (2, 1, left))]
    x_loads[0].wait()
    _each(0, half // strip, norm)
    _greeted()
    own_copies[0].start()
    x_loads[1].wait()
    _each(half // strip, rows // strip, norm)
    _start(own_copies[1:])

    first = lax.broadcasted_iota(jnp.int32, (rows, HEAD), 1) < HEAD // 2
    for block in range(n):
        table_load(block).wait()
        both = cos_s[block]
        other = pltpu.roll(both, HEAD // 2, 1)
        cos_s[block] = jnp.where(first, both, other)
        sin_s[block] = jnp.where(first, -other, both)
    top_s[...] = jnp.full(top_s.shape, NEG, F32)
    mix_s[...] = jnp.zeros(mix_s.shape, F32)
    v_s[:, :, HEAD:, :] = jnp.ones((kv, n, 8, rows), BF16)

    def turned(t, block):
        t = t.astype(BF16).astype(F32)
        return (t * cos_s[block] + pltpu.roll(t, HEAD // 2, 1) * sin_s[block]).astype(BF16)

    def project(blocks, last):
        def one(j):
            @pl.when(j < q_tiles - 2)
            def _():
                q_load(j + 2).start()

            for i in range(2):
                @pl.when(j == q_tiles - 2 + i)
                def _():
                    kv_load(i).start()

            q_load(j).wait()
            for block in blocks:
                t = _dot(b_s[block], w_s[lax.rem(j, 3)])
                for i in range(TILE // HEAD):
                    q_s[j * (TILE // HEAD) + i, block] = turned(t[:, i * HEAD : (i + 1) * HEAD], block)

        _each(0, q_tiles, one)
        for i in range(2):
            if not last:
                q_load(i).start()
            kv_load(i).wait()
            for block in blocks:
                t = _dot(b_s[block], w_s[(q_tiles + i) % 3])
                for g in range(kv):
                    some = t[:, g * HEAD : (g + 1) * HEAD]
                    if i == 0:
                        k_s[g, block] = turned(some, block)
                    else:
                        v_s[g, block, :HEAD, :] = some.astype(BF16).T

    def score(g, iq, j, masked):
        keys, values, state = k_s[g, j], v_s[g, j], g * n + iq
        scores = [_dot(keys, q_s[g * group + h, iq], 1, 1) for h in range(group)]
        weights, keeps = [], []
        if masked:
            seen = lax.broadcasted_iota(jnp.int32, (rows, rows), 1) >= lax.broadcasted_iota(jnp.int32, (rows, rows), 0)
        for h, s in enumerate(scores):
            at = pl.ds(h * rows, rows)
            if masked:
                s = jnp.where(seen, s, HIDDEN)
            old = top_s[state, :, at]
            top = jnp.maximum(old, s.max(axis=0, keepdims=True))
            top_s[state, :, at] = top
            weights.append(jnp.exp2((s - top) * e).astype(BF16))
            keeps.append(jnp.exp2((old - top) * e))
        for h, (p, keep) in enumerate(zip(weights, keeps)):
            at = pl.ds(h * rows, rows)
            mix_s[state, :, at] = mix_s[state, :, at] * keep + _dot(values, p)

    def pairs(count, which):
        def one(t):
            iq, j = which(lax.rem(t, count))

            @pl.when(place(j) < place(iq))
            def _():
                score(t // count, iq, j, False)

        _each(0, kv * count, one)

    def finish(block):
        for g in range(kv):
            for h in range(group):
                at = pl.ds(h * rows, rows)
                state = g * n + block
                o_s[block, :, pl.ds((g * group + h) * HEAD, HEAD)] = (
                    mix_s[state, :HEAD, at] * (1 / mix_s[state, HEAD : HEAD + 1, at])).T.astype(BF16)

    def store(block):
        return pltpu.make_async_copy(o_s.at[block], out.at[pl.ds(block * rows, rows), :], o_sem.at[block])

    project([own], False)
    for c in own_copies[:2]:
        c.wait_recv()
    _start(forwards)
    for c in own_copies[2:]:
        c.wait_recv()
    project([1, 2], False)
    near = n - 1
    _each(0, kv * near, lambda t: score(t // near, lax.rem(t, near), lax.rem(t, near), True))
    pairs(near * near, lambda t: (t // near, lax.rem(t, near)))
    for c in forwards:
        c.wait_recv()
    project([far], True)
    _each(0, kv, lambda g: score(g, far, far, True))
    pairs(2 * near, lambda t: (jnp.where(t < near, far, t - near), jnp.where(t < near, t, far)))
    for block in range(n):
        finish(block)
        store(block).start()
    for c in own_copies + forwards:
        c.wait_send()
    for block in range(n):
        store(block).wait()


def head(n, x, gains, wq, wk, wv):
    rows, d = x.shape
    heads, kv = wq.shape[1] // HEAD, wk.shape[1] // HEAD
    half = HEAD // 2
    angle = np.arange(n * rows, dtype=np.float32)[:, None] * np.float32(THETA) ** (-np.arange(half, dtype=np.float32) / np.float32(half))
    table = np.concatenate([np.cos(angle), np.sin(angle)], -1).astype(np.float32).reshape(n, rows, HEAD)
    hbm, vmem = pl.BlockSpec(memory_space=pl.ANY), pl.BlockSpec(memory_space=pltpu.VMEM)
    dma = pltpu.SemaphoreType.DMA
    return pl.pallas_call(
        functools.partial(_head_kernel, n, heads, kv),
        in_specs=[hbm, vmem, hbm, hbm, hbm, hbm],
        out_specs=hbm,
        out_shape=jax.ShapeDtypeStruct((n * rows, heads * HEAD), BF16),
        scratch_shapes=[
            pltpu.VMEM((n, rows, d), BF16),
            pltpu.VMEM((3, d, TILE), BF16),
            pltpu.VMEM((heads, n, rows, HEAD), BF16),
            pltpu.VMEM((kv, n, rows, HEAD), BF16),
            pltpu.VMEM((kv, n, HEAD + 8, rows), BF16),
            pltpu.VMEM((n, rows, HEAD), F32),
            pltpu.VMEM((n, rows, HEAD), F32),
            pltpu.VMEM((kv * n, 1, heads // kv * rows), F32),
            pltpu.VMEM((kv * n, HEAD + 8, heads // kv * rows), F32),
            pltpu.VMEM((n, rows, heads * HEAD), BF16),
            dma((2,)), dma((3,)), dma((n,)), dma((n,)), dma((n, 2)), dma((n, 2)),
        ],
        compiler_params=pltpu.CompilerParams(collective_id=1, has_side_effects=True, vmem_limit_bytes=60 * 2**20),
        cost_estimate=pl.CostEstimate(flops=2 * n * rows * d * (wq.shape[1] + 2 * wk.shape[1]), transcendentals=heads * (n * rows) ** 2,
                                      bytes_accessed=6 * d * (wq.shape[1] + 2 * wk.shape[1])),
    )(x, gains, jnp.asarray(table), wq, wk, wv)


GROUP = 512
LAG = 4


def _tail_kernel(n, seen, x, gain, wo, wg, wu, wd, y, hid_s, b_s, h_s, w_s, via_s, near_s, own_s, part_s, far_s, send_s, ss_s, acc_s,
                 load_sem, x_sem, w_sem, far_sem, send_sem, via_sem, near_sem, ag_send, ag_recv):
    right, left = _neighbours(n)
    p_rows = h_s.shape[1]
    half = p_rows // 2
    all_rows, d = b_s.shape[1], b_s.shape[2]
    groups = d // GROUP
    wo_k, ff = wo.shape[0], wd.shape[0]
    rows_here = x.shape[0]
    tiles = ff // 128
    part = all_rows // 2

    _greet((left, right))

    def loads(p):
        at = [seen.at[pl.ds(i * rows_here + p * p_rows, p_rows), :] for i in (3, 1, 2, 0)]
        return [pltpu.make_async_copy(src, hid_s.at[pl.ds(i * p_rows, p_rows), pl.ds(p * wo_k, wo_k)], load_sem.at[p, i])
                for i, src in enumerate(at)]

    def x_load(p):
        return pltpu.make_async_copy(x.at[pl.ds(p * p_rows, p_rows), :], h_s.at[p], x_sem.at[p])

    def y_store(p):
        return pltpu.make_async_copy(h_s.at[p], y.at[pl.ds(p * p_rows, p_rows), :], x_sem.at[p])

    def wo_load(g, slot):
        return [pltpu.make_async_copy(wo.at[:, _columns(g * (GROUP // TILE) + s, TILE)], w_s.at[slot, pl.ds(s * wo_k, wo_k), :],
                                      w_sem.at[slot, s]) for s in range(GROUP // TILE)]

    def gu_load(k, slot):
        return [pltpu.make_async_copy(w.at[:, _columns(k, 128)], w_s.at[slot, :, pl.ds(i * 128, 128)], w_sem.at[slot, i])
                for i, w in enumerate((wg, wu))]

    def wd_load(m, slot):
        return [pltpu.make_async_copy(wd.at[:, _columns(m, TILE)], w_s.at[slot, pl.ds(0, ff), :], w_sem.at[slot, 0])]

    def far_copies(p, g):
        return [_remote(far_s.at[g, pl.ds(i * half, half), :], via_s.at[p, g, pl.ds(i * half, half), :], far_sem.at[g, i],
                       via_sem.at[p, g, i], to) for i, to in enumerate((right, left))]

    def near_copies(p, g):
        return [_remote(send_s.at[g, i], near_s.at[p, i, g], send_sem.at[g, i], near_sem.at[p, g, i], to)
                for i, to in enumerate((right, left))]

    def keep(g, s, i, acc):
        cols = pl.ds(s * TILE, TILE)
        first, second = acc[:p_rows], acc[p_rows:]
        if i == 0:
            far_s[g, :, cols] = first.astype(BF16)
            part_s[g, pl.ds(p_rows, p_rows), cols] = second
        else:
            part_s[g, pl.ds(0, p_rows), cols] = first
            own_s[g, :, cols] = second

    def pass_on(p, g):
        for c in far_copies(p, g):
            c.wait_recv()
        send_s[g, 0, pl.ds(0, half), :] = (part_s[g, pl.ds(0, half), :] + via_s[p, g, pl.ds(0, half), :].astype(F32)).astype(BF16)
        send_s[g, 0, pl.ds(half, half), :] = part_s[g, pl.ds(half, half), :].astype(BF16)
        send_s[g, 1, pl.ds(0, half), :] = part_s[g, pl.ds(2 * half, half), :].astype(BF16)
        send_s[g, 1, pl.ds(half, half), :] = (part_s[g, pl.ds(3 * half, half), :] + via_s[p, g, pl.ds(half, half), :].astype(F32)).astype(BF16)
        _start(near_copies(p, g))

    def add_up(p, g, norm):
        for c in near_copies(p, g):
            c.wait_recv()
        cols = _columns(g, GROUP)
        total = own_s[g] + near_s[p, 0, g].astype(F32) + near_s[p, 1, g].astype(F32)
        h = (h_s[p, :, cols].astype(F32) + total).astype(BF16)
        h_s[p, :, cols] = h
        if norm:
            h = h.astype(F32)
            h = h * h
            ss_s[...] += sum(h[:, i * 128 : (i + 1) * 128] for i in range(GROUP // 128))

    def sent(p):
        def one(g, _):
            for c in far_copies(p, g) + near_copies(p, g):
                c.wait_send()
        lax.fori_loop(0, groups, one, None)

    def scale_rows(p):
        scale = lax.rsqrt(jnp.sum(ss_s[...], -1, keepdims=True) / d + 1e-6)

        def one(g, _):
            cols = _columns(g, GROUP)
            b_s[p, pl.ds(3 * p_rows, p_rows), cols] = (h_s[p, :, cols].astype(F32) * scale * gain[1:2, cols]).astype(BF16)

        lax.fori_loop(0, groups, one, None)
        ss_s[...] = jnp.zeros(ss_s.shape, F32)

    def rows_of(p, block, i):
        return b_s.at[p, pl.ds(block * p_rows + i * half, half), :]

    def own_copies(p):
        return [_remote(rows_of(p, 3, i), rows_of(p, block, i), ag_send.at[p, block, i], ag_recv.at[p, block, i], to)
                for block, i, to in ((1, 0, right), (2, 1, left), (1, 1, right), (2, 0, left))]

    def forwards(p):
        return [_remote(rows_of(p, block, i), rows_of(p, 0, i), ag_send.at[p, 0, i], ag_recv.at[p, 0, i], to)
                for block, i, to in ((1, 0, right), (2, 1, left))]

    def forward(p):
        for c in own_copies(p)[:2]:
            c.wait_recv()
        _start(forwards(p))

    def gathered(p):
        for c in own_copies(p)[2:] + forwards(p):
            c.wait_recv()

    def out_project(p):
        def one(g, _):
            slot = lax.rem(g, 2)

            @pl.when(g + 1 < groups)
            def _():
                _start(wo_load(g + 1, 1 - slot))

            _wait(wo_load(g, slot))
            for s in range(GROUP // TILE):
                for i in range(2):
                    keep(g, s, i, jnp.dot(hid_s[pl.ds(i * part, part), pl.ds(p * wo_k, wo_k)], w_s[slot, pl.ds(s * wo_k, wo_k), :],
                                          preferred_element_type=F32))
            _start(far_copies(p, g))
            if p == 0:
                @pl.when(g >= LAG)
                def _():
                    pass_on(p, g - LAG)

        lax.fori_loop(0, groups, one, None)

    def gate_up(p, beside):
        def one(k, _):
            slot = lax.rem(k, 2)

            @pl.when(k + 1 < tiles)
            def _():
                _start(gu_load(k + 1, 1 - slot))

            @pl.when(k + 1 == tiles)
            def _():
                _start(wd_load(0, 0))

            _wait(gu_load(k, slot))
            activate(k - 1, 1 - slot)
            for i in range(2):
                acc_s[slot, pl.ds(i * part, part), :] = jnp.dot(b_s[p, pl.ds(i * part, part), :], w_s[slot], preferred_element_type=F32)
            beside(k)

        def activate(k, slot):
            gate, up = acc_s[slot, :, :128], acc_s[slot, :, 128:]
            hid_s[:, _columns(jnp.maximum(k, 0), 128)] = (gate * lax.logistic(gate) * up).astype(BF16)

        lax.fori_loop(0, tiles, one, None)
        activate(tiles - 1, (tiles - 1) % 2)

    def down(p):
        steps = GROUP // TILE

        def one(g, _):
            for s in range(steps):
                m = g * steps + s
                if s + 1 < steps:
                    _start(wd_load(m + 1, (s + 1) % 2))
                else:
                    @pl.when(g + 1 < groups)
                    def _():
                        _start(wd_load(m + 1, (s + 1) % 2))

                    if p == 0:
                        @pl.when(g + 1 == groups)
                        def _():
                            _start(gu_load(0, 0))

                _wait(wd_load(m, s % 2))
                for i in range(2):
                    keep(g, s, i, jnp.dot(hid_s[pl.ds(i * part, part), :], w_s[s % 2, pl.ds(0, ff), :], preferred_element_type=F32))
            _start(far_copies(p, g))
            if p == 1:
                @pl.when(g >= LAG)
                def _():
                    pass_on(p, g - LAG)

        lax.fori_loop(0, groups, one, None)

    _start(wo_load(0, 0))
    for p in range(2):
        _start(loads(p))
        x_load(p).start()
    ss_s[...] = jnp.zeros(ss_s.shape, F32)
    _greeted()

    _wait(loads(0))
    out_project(0)
    _start(wo_load(0, 0))
    _each(groups - LAG, groups, lambda g: pass_on(0, g))
    x_load(0).wait()
    _each(0, groups, lambda g: add_up(0, g, True))
    sent(0)
    scale_rows(0)
    _start(own_copies(0))
    forward(0)
    _wait(loads(1))
    out_project(1)
    _start(gu_load(0, 0))
    x_load(1).wait()
    gathered(0)

    def beside_first(k):
        @pl.when(k < groups)
        def _():
            pass_on(1, k)

        @pl.when((k >= groups) & (k < 2 * groups))
        def _():
            add_up(1, k - groups, True)

        @pl.when(k == 2 * groups)
        def _():
            sent(1)
            scale_rows(1)
            _start(own_copies(1))

        @pl.when(k == tiles - 2)
        def _():
            forward(1)

    gate_up(0, beside_first)
    down(0)
    gathered(1)

    def beside_second(k):
        @pl.when(k < groups)
        def _():
            pass_on(0, k)

        @pl.when((k >= groups) & (k < 2 * groups))
        def _():
            add_up(0, k - groups, False)

    gate_up(1, beside_second)
    sent(0)
    y_store(0).start()
    down(1)
    _each(groups - LAG, groups, lambda g: pass_on(1, g))
    _each(0, groups, lambda g: add_up(1, g, False))
    y_store(1).start()
    sent(1)
    for p in range(2):
        for c in own_copies(p) + forwards(p):
            c.wait_send()
        y_store(p).wait()


def tail(n, seen, x, gains, wo, wg, wu, wd):
    rows, d = x.shape
    p_rows = rows // 2
    groups, ff = d // GROUP, wd.shape[0]
    dma = pltpu.SemaphoreType.DMA
    hbm = pl.BlockSpec(memory_space=pl.ANY)
    return pl.pallas_call(
        functools.partial(_tail_kernel, n),
        in_specs=[hbm, hbm, pl.BlockSpec(memory_space=pltpu.VMEM), hbm, hbm, hbm, hbm],
        out_specs=hbm,
        out_shape=jax.ShapeDtypeStruct(x.shape, BF16),
        scratch_shapes=[
            pltpu.VMEM((n * p_rows, ff), BF16),
            pltpu.VMEM((2, n * p_rows, d), BF16),
            pltpu.VMEM((2, p_rows, d), BF16),
            pltpu.VMEM((2, d, TILE), BF16),
            pltpu.VMEM((2, groups, p_rows, GROUP), BF16),
            pltpu.VMEM((2, 2, groups, p_rows, GROUP), BF16),
            pltpu.VMEM((groups, p_rows, GROUP), F32),
            pltpu.VMEM((groups, 2 * p_rows, GROUP), F32),
            pltpu.VMEM((groups, p_rows, GROUP), BF16),
            pltpu.VMEM((groups, 2, p_rows, GROUP), BF16),
            pltpu.VMEM((p_rows, 128), F32),
            pltpu.VMEM((2, n * p_rows, TILE), F32),
            dma((2, n)), dma((2,)), dma((2, 2)), dma((groups, 2)), dma((groups, 2)), dma((2, groups, 2)), dma((2, groups, 2)),
            dma((2, 3, 2)), dma((2, 3, 2)),
        ],
        compiler_params=pltpu.CompilerParams(collective_id=0, has_side_effects=True, vmem_limit_bytes=67043328),
        cost_estimate=pl.CostEstimate(flops=2 * n * rows * d * (wo.shape[0] + 3 * ff), transcendentals=n * rows * ff,
                                      bytes_accessed=2 * d * (wo.shape[0] + 6 * ff)),
    )(seen, x, gains, wo, wg, wu, wd)


def solution(mesh):
    n = mesh.shape["tp"]

    def step(x, gain_a, wq, wk, wv, wo, gain_m, w_gate, w_up, w_down):
        gains = jnp.stack([gain_a, gain_m]).astype(F32)
        return tail(n, head(n, x, gains, wq, wk, wv), x, gains, wo, w_gate, w_up, w_down)

    tokens, columns, rows_of = P(("dp", "tp"), None), P(None, "tp"), P("tp", None)
    return jax.shard_map(
        step,
        mesh=mesh,
        in_specs=(tokens, P(None), columns, columns, columns, rows_of, P(None), columns, columns, rows_of),
        out_specs=tokens,
        check_vma=False,
    )
```

```python
import functools

import jax
import jax.numpy as jnp
import numpy as np
from jax import lax
from jax.experimental import pallas as pl
from jax.experimental.pallas import tpu as pltpu
from jax.sharding import PartitionSpec as P

HEAD = 128
THETA = 10000
NEG = -1e30
HIDDEN = 2 * NEG
LOG2E = 1.4426950408889634
BF16, F32 = jnp.bfloat16, jnp.float32


MESH = pl.DeviceIdType.MESH
TILE = 256


def _columns(i, size):
    return pl.ds(pl.multiple_of(i * size, size), size)


def _neighbours(n):
    me = lax.axis_index("tp")
    return {"tp": lax.rem(me + 1, n)}, {"tp": lax.rem(me + n - 1, n)}


def _greet(neighbours):
    barrier = pltpu.get_barrier_semaphore()
    for neighbour in neighbours:
        pl.semaphore_signal(barrier, inc=1, device_id=neighbour, device_id_type=MESH)


def _greeted():
    pl.semaphore_wait(pltpu.get_barrier_semaphore(), 2)


def _remote(src, dst, s_sem, r_sem, to):
    return pltpu.make_async_remote_copy(src_ref=src, dst_ref=dst, send_sem=s_sem, recv_sem=r_sem, device_id=to, device_id_type=MESH)


def _start(copies):
    for c in copies:
        c.start()


def _wait(copies):
    for c in copies:
        c.wait()


def _each(lo, hi, do):
    lax.fori_loop(lo, hi, lambda i, _: do(i), None)


def _dot(a, b, ca=1, cb=0):
    return lax.dot_general(a, b, (((ca,), (cb,)), ((), ())), preferred_element_type=F32)


def _head_kernel(n, heads, kv, x, gain, table, wq, wk, wv, out, b_s, w_s, q_s, k_s, v_s, cos_s, sin_s, top_s, mix_s, o_s,
                 x_sem, w_sem, o_sem, t_sem, ag_send, ag_recv):
    right, left = _neighbours(n)
    me = lax.axis_index("tp")
    rows, d = x.shape
    half, group = rows // 2, heads // kv
    q_tiles = heads * HEAD // TILE
    e = HEAD**-0.5 * LOG2E
    own, far = 0, n - 1

    def place(block):
        step = jnp.where(block == 0, 0, jnp.where(block == 1, n - 1, block - 1))
        return lax.rem(me + step, n)

    _greet((left, right))
    x_loads = [pltpu.make_async_copy(x.at[pl.ds(i * half, half), :], b_s.at[own, pl.ds(i * half, half), :], x_sem.at[i]) for i in range(2)]
    _start(x_loads)

    def table_load(block):
        return pltpu.make_async_copy(table.at[place(block)], cos_s.at[block], t_sem.at[block])


    def q_load(j):
        return pltpu.make_async_copy(wq.at[:, _columns(j, TILE)], w_s.at[lax.rem(j, 3)], w_sem.at[lax.rem(j, 3)])

    def kv_load(i):
        slot = (q_tiles + i) % 3
        return pltpu.make_async_copy((wk, wv)[i], w_s.at[slot], w_sem.at[slot])

    for block in range(n):
        table_load(block).start()
    q_load(0).start()
    q_load(1).start()

    strip = 16

    def norm(i):
        at = pl.ds(pl.multiple_of(i * strip, strip), strip)
        wide = b_s[own, at, :].astype(F32)
        scale = lax.rsqrt(jnp.mean(wide * wide, -1, keepdims=True) + 1e-6)
        b_s[own, at, :] = (wide * scale * gain[0:1, :]).astype(BF16)

    def part(block, i):
        return b_s.at[block, pl.ds(i * half, half), :]

    own_copies = [_remote(part(own, i), part(block, i), ag_send.at[block, i], ag_recv.at[block, i], to)
                  for block, i, to in ((1, 0, right), (2, 1, left), (1, 1, right), (2, 0, left))]
    forwards = [_remote(part(block, i), part(far, i), ag_send.at[far, i], ag_recv.at[far, i], to)
                for block, i, to in ((1, 0, right), (2, 1, left))]
    x_loads[0].wait()
    _each(0, half // strip, norm)
    _greeted()
    own_copies[0].start()
    x_loads[1].wait()
    _each(half // strip, rows // strip, norm)
    _start(own_copies[1:])

    first = lax.broadcasted_iota(jnp.int32, (rows, HEAD), 1) < HEAD // 2
    for block in range(n):
        table_load(block).wait()
        both = cos_s[block]
        other = pltpu.roll(both, HEAD // 2, 1)
        cos_s[block] = jnp.where(first, both, other)
        sin_s[block] = jnp.where(first, -other, both)
    top_s[...] = jnp.full(top_s.shape, NEG, F32)
    mix_s[...] = jnp.zeros(mix_s.shape, F32)
    v_s[:, :, HEAD:, :] = jnp.ones((kv, n, 8, rows), BF16)

    def turned(t, block):
        t = t.astype(BF16).astype(F32)
        return (t * cos_s[block] + pltpu.roll(t, HEAD // 2, 1) * sin_s[block]).astype(BF16)

    def project(blocks, last):
        def products(slot):
            t = _dot(b_s[pl.ds(blocks[0], len(blocks))].reshape(len(blocks) * rows, d), w_s[slot])
            return [(block, t[i * rows : (i + 1) * rows]) for i, block in enumerate(blocks)]

        def one(j):
            @pl.when(j < q_tiles - 2)
            def _():
                q_load(j + 2).start()

            for i in range(2):
                @pl.when(j == q_tiles - 2 + i)
                def _():
                    kv_load(i).start()

            q_load(j).wait()
            for block, t in products(lax.rem(j, 3)):
                for i in range(TILE // HEAD):
                    q_s[j * (TILE // HEAD) + i, block] = turned(t[:, i * HEAD : (i + 1) * HEAD], block)

        _each(0, q_tiles, one)
        for i in range(2):
            if not last:
                q_load(i).start()
            kv_load(i).wait()
            for block, t in products((q_tiles + i) % 3):
                for g in range(kv):
                    some = t[:, g * HEAD : (g + 1) * HEAD]
                    if i == 0:
                        k_s[g, block] = turned(some, block)
                    else:
                        v_s[g, block, :HEAD, :] = some.astype(BF16).T

    def score(g, iq, j, masked):
        keys, values, state = k_s[g, j], v_s[g, j], g * n + iq
        scores = [_dot(keys, q_s[g * group + h, iq], 1, 1) for h in range(group)]
        weights, keeps = [], []
        if masked:
            seen = lax.broadcasted_iota(jnp.int32, (rows, rows), 1) >= lax.broadcasted_iota(jnp.int32, (rows, rows), 0)
        for h, s in enumerate(scores):
            at = pl.ds(h * rows, rows)
            if masked:
                s = jnp.where(seen, s, HIDDEN)
            old = top_s[state, :, at]
            top = jnp.maximum(old, s.max(axis=0, keepdims=True))
            top_s[state, :, at] = top
            weights.append(jnp.exp2((s - top) * e).astype(BF16))
            keeps.append(jnp.exp2((old - top) * e))
        for h, (p, keep) in enumerate(zip(weights, keeps)):
            at = pl.ds(h * rows, rows)
            mix_s[state, :, at] = mix_s[state, :, at] * keep + _dot(values, p)

    def pairs(count, which):
        def one(t):
            iq, j = which(lax.rem(t, count))

            @pl.when(place(j) < place(iq))
            def _():
                score(t // count, iq, j, False)

        _each(0, kv * count, one)

    def finish(block):
        for g in range(kv):
            for h in range(group):
                at = pl.ds(h * rows, rows)
                state = g * n + block
                o_s[block, :, pl.ds((g * group + h) * HEAD, HEAD)] = (
                    mix_s[state, :HEAD, at] * (1 / mix_s[state, HEAD : HEAD + 1, at])).T.astype(BF16)

    def store(block):
        return pltpu.make_async_copy(o_s.at[block], out.at[pl.ds(block * rows, rows), :], o_sem.at[block])

    project([own], False)
    for c in own_copies[:2]:
        c.wait_recv()
    _start(forwards)
    for c in own_copies[2:]:
        c.wait_recv()
    project([1, 2], False)
    near = n - 1
    _each(0, kv * near, lambda t: score(t // near, lax.rem(t, near), lax.rem(t, near), True))
    pairs(near * near, lambda t: (t // near, lax.rem(t, near)))
    for c in forwards:
        c.wait_recv()
    project([far], True)
    _each(0, kv, lambda g: score(g, far, far, True))
    pairs(2 * near, lambda t: (jnp.where(t < near, far, t - near), jnp.where(t < near, t, far)))
    for block in range(n):
        finish(block)
        store(block).start()
    for c in own_copies + forwards:
        c.wait_send()
    for block in range(n):
        store(block).wait()


def head(n, x, gains, wq, wk, wv):
    rows, d = x.shape
    heads, kv = wq.shape[1] // HEAD, wk.shape[1] // HEAD
    half = HEAD // 2
    angle = np.arange(n * rows, dtype=np.float32)[:, None] * np.float32(THETA) ** (-np.arange(half, dtype=np.float32) / np.float32(half))
    table = np.concatenate([np.cos(angle), np.sin(angle)], -1).astype(np.float32).reshape(n, rows, HEAD)
    hbm, vmem = pl.BlockSpec(memory_space=pl.ANY), pl.BlockSpec(memory_space=pltpu.VMEM)
    dma = pltpu.SemaphoreType.DMA
    return pl.pallas_call(
        functools.partial(_head_kernel, n, heads, kv),
        in_specs=[hbm, vmem, hbm, hbm, hbm, hbm],
        out_specs=hbm,
        out_shape=jax.ShapeDtypeStruct((n * rows, heads * HEAD), BF16),
        scratch_shapes=[
            pltpu.VMEM((n, rows, d), BF16),
            pltpu.VMEM((3, d, TILE), BF16),
            pltpu.VMEM((heads, n, rows, HEAD), BF16),
            pltpu.VMEM((kv, n, rows, HEAD), BF16),
            pltpu.VMEM((kv, n, HEAD + 8, rows), BF16),
            pltpu.VMEM((n, rows, HEAD), F32),
            pltpu.VMEM((n, rows, HEAD), F32),
            pltpu.VMEM((kv * n, 1, heads // kv * rows), F32),
            pltpu.VMEM((kv * n, HEAD + 8, heads // kv * rows), F32),
            pltpu.VMEM((n, rows, heads * HEAD), BF16),
            dma((2,)), dma((3,)), dma((n,)), dma((n,)), dma((n, 2)), dma((n, 2)),
        ],
        compiler_params=pltpu.CompilerParams(collective_id=1, has_side_effects=True, vmem_limit_bytes=60 * 2**20),
        cost_estimate=pl.CostEstimate(flops=2 * n * rows * d * (wq.shape[1] + 2 * wk.shape[1]), transcendentals=heads * (n * rows) ** 2,
                                      bytes_accessed=6 * d * (wq.shape[1] + 2 * wk.shape[1])),
    )(x, gains, jnp.asarray(table), wq, wk, wv)


GROUP = 512
LAG = 4


def _tail_kernel(n, seen, x, gain, wo, wg, wu, wd, y, hid_s, b_s, h_s, w_s, via_s, near_s, own_s, part_s, far_s, send_s, ss_s, acc_s,
                 load_sem, x_sem, w_sem, far_sem, send_sem, via_sem, near_sem, ag_send, ag_recv):
    right, left = _neighbours(n)
    p_rows = h_s.shape[1]
    half = p_rows // 2
    all_rows, d = b_s.shape[1], b_s.shape[2]
    groups = d // GROUP
    wo_k, ff = wo.shape[0], wd.shape[0]
    rows_here = x.shape[0]
    tiles = ff // 128

    _greet((left, right))

    def loads(p):
        at = [seen.at[pl.ds(i * rows_here + p * p_rows, p_rows), :] for i in (3, 1, 2, 0)]
        return [pltpu.make_async_copy(src, hid_s.at[pl.ds(i * p_rows, p_rows), pl.ds(p * wo_k, wo_k)], load_sem.at[p, i])
                for i, src in enumerate(at)]

    def x_load(p):
        return pltpu.make_async_copy(x.at[pl.ds(p * p_rows, p_rows), :], h_s.at[p], x_sem.at[p])

    def y_store(p):
        return pltpu.make_async_copy(h_s.at[p], y.at[pl.ds(p * p_rows, p_rows), :], x_sem.at[p])

    def wo_load(g, slot):
        return [pltpu.make_async_copy(wo.at[:, _columns(g * (GROUP // TILE) + s, TILE)], w_s.at[slot, pl.ds(s * wo_k, wo_k), :],
                                      w_sem.at[slot, s]) for s in range(GROUP // TILE)]

    def gu_load(k, slot):
        return [pltpu.make_async_copy(w.at[:, _columns(k, 128)], w_s.at[slot, :, pl.ds(i * 128, 128)], w_sem.at[slot, i])
                for i, w in enumerate((wg, wu))]

    def wd_load(m, slot):
        return [pltpu.make_async_copy(wd.at[:, _columns(m, TILE)], w_s.at[slot, pl.ds(0, ff), :], w_sem.at[slot, 0])]

    def far_copies(p, g):
        return [_remote(far_s.at[g, pl.ds(i * half, half), :], via_s.at[p, g, pl.ds(i * half, half), :], far_sem.at[g, i],
                       via_sem.at[p, g, i], to) for i, to in enumerate((right, left))]

    def near_copies(p, g):
        return [_remote(send_s.at[g, i], near_s.at[p, i, g], send_sem.at[g, i], near_sem.at[p, g, i], to)
                for i, to in enumerate((right, left))]

    def keep(g, s, acc):
        cols = pl.ds(s * TILE, TILE)
        far_s[g, :, cols] = acc[:p_rows].astype(BF16)
        part_s[g, pl.ds(p_rows, p_rows), cols] = acc[p_rows : 2 * p_rows]
        part_s[g, pl.ds(0, p_rows), cols] = acc[2 * p_rows : 3 * p_rows]
        own_s[g, :, cols] = acc[3 * p_rows :]

    def pass_on(p, g):
        for c in far_copies(p, g):
            c.wait_recv()
        send_s[g, 0, pl.ds(0, half), :] = (part_s[g, pl.ds(0, half), :] + via_s[p, g, pl.ds(0, half), :].astype(F32)).astype(BF16)
        send_s[g, 0, pl.ds(half, half), :] = part_s[g, pl.ds(half, half), :].astype(BF16)
        send_s[g, 1, pl.ds(0, half), :] = part_s[g, pl.ds(2 * half, half), :].astype(BF16)
        send_s[g, 1, pl.ds(half, half), :] = (part_s[g, pl.ds(3 * half, half), :] + via_s[p, g, pl.ds(half, half), :].astype(F32)).astype(BF16)
        _start(near_copies(p, g))

    def add_up(p, g, norm):
        for c in near_copies(p, g):
            c.wait_recv()
        cols = _columns(g, GROUP)
        total = own_s[g] + near_s[p, 0, g].astype(F32) + near_s[p, 1, g].astype(F32)
        h = (h_s[p, :, cols].astype(F32) + total).astype(BF16)
        h_s[p, :, cols] = h
        if norm:
            h = h.astype(F32)
            h = h * h
            ss_s[...] += sum(h[:, i * 128 : (i + 1) * 128] for i in range(GROUP // 128))

    def sent(p):
        def one(g, _):
            for c in far_copies(p, g) + near_copies(p, g):
                c.wait_send()
        lax.fori_loop(0, groups, one, None)

    def scale_rows(p):
        scale = lax.rsqrt(jnp.sum(ss_s[...], -1, keepdims=True) / d + 1e-6)

        def one(g, _):
            cols = _columns(g, GROUP)
            b_s[p, pl.ds(3 * p_rows, p_rows), cols] = (h_s[p, :, cols].astype(F32) * scale * gain[1:2, cols]).astype(BF16)

        lax.fori_loop(0, groups, one, None)
        ss_s[...] = jnp.zeros(ss_s.shape, F32)

    def rows_of(p, block, i):
        return b_s.at[p, pl.ds(block * p_rows + i * half, half), :]

    def own_copies(p):
        return [_remote(rows_of(p, 3, i), rows_of(p, block, i), ag_send.at[p, block, i], ag_recv.at[p, block, i], to)
                for block, i, to in ((1, 0, right), (2, 1, left), (1, 1, right), (2, 0, left))]

    def forwards(p):
        return [_remote(rows_of(p, block, i), rows_of(p, 0, i), ag_send.at[p, 0, i], ag_recv.at[p, 0, i], to)
                for block, i, to in ((1, 0, right), (2, 1, left))]

    def forward(p):
        for c in own_copies(p)[:2]:
            c.wait_recv()
        _start(forwards(p))

    def gathered(p):
        for c in own_copies(p)[2:] + forwards(p):
            c.wait_recv()

    def out_project(p):
        def one(g, _):
            slot = lax.rem(g, 2)

            @pl.when(g + 1 < groups)
            def _():
                _start(wo_load(g + 1, 1 - slot))

            _wait(wo_load(g, slot))
            for s in range(GROUP // TILE):
                keep(g, s, _dot(hid_s[:, pl.ds(p * wo_k, wo_k)], w_s[slot, pl.ds(s * wo_k, wo_k), :]))
            _start(far_copies(p, g))
            if p == 0:
                @pl.when(g >= LAG)
                def _():
                    pass_on(p, g - LAG)

        lax.fori_loop(0, groups, one, None)

    def gate_up(p, beside):
        def one(k, _):
            slot = lax.rem(k, 2)

            @pl.when(k + 1 < tiles)
            def _():
                _start(gu_load(k + 1, 1 - slot))

            @pl.when(k + 1 == tiles)
            def _():
                _start(wd_load(0, 0))

            _wait(gu_load(k, slot))
            activate(k - 1, 1 - slot)
            acc_s[slot] = _dot(b_s[p], w_s[slot])
            beside(k)

        def activate(k, slot):
            gate, up = acc_s[slot, :, :128], acc_s[slot, :, 128:]
            hid_s[:, _columns(jnp.maximum(k, 0), 128)] = (gate * lax.logistic(gate) * up).astype(BF16)

        lax.fori_loop(0, tiles, one, None)
        activate(tiles - 1, (tiles - 1) % 2)

    def down(p):
        steps = GROUP // TILE

        def one(g, _):
            for s in range(steps):
                m = g * steps + s
                if s + 1 < steps:
                    _start(wd_load(m + 1, (s + 1) % 2))
                else:
                    @pl.when(g + 1 < groups)
                    def _():
                        _start(wd_load(m + 1, (s + 1) % 2))

                    if p == 0:
                        @pl.when(g + 1 == groups)
                        def _():
                            _start(gu_load(0, 0))

                _wait(wd_load(m, s % 2))
                keep(g, s, _dot(hid_s[...], w_s[s % 2, pl.ds(0, ff), :]))
            _start(far_copies(p, g))
            if p == 1:
                @pl.when(g >= LAG)
                def _():
                    pass_on(p, g - LAG)

        lax.fori_loop(0, groups, one, None)

    _start(wo_load(0, 0))
    for p in range(2):
        _start(loads(p))
        x_load(p).start()
    ss_s[...] = jnp.zeros(ss_s.shape, F32)
    _greeted()

    _wait(loads(0))
    out_project(0)
    _start(wo_load(0, 0))
    _each(groups - LAG, groups, lambda g: pass_on(0, g))
    x_load(0).wait()
    _each(0, groups, lambda g: add_up(0, g, True))
    sent(0)
    scale_rows(0)
    _start(own_copies(0))
    forward(0)
    _wait(loads(1))
    out_project(1)
    _start(gu_load(0, 0))
    x_load(1).wait()
    gathered(0)

    def beside_first(k):
        @pl.when(k < groups)
        def _():
            pass_on(1, k)

        @pl.when((k >= groups) & (k < 2 * groups))
        def _():
            add_up(1, k - groups, True)

        @pl.when(k == 2 * groups)
        def _():
            sent(1)
            scale_rows(1)
            _start(own_copies(1))

        @pl.when(k == tiles - 2)
        def _():
            forward(1)

    gate_up(0, beside_first)
    down(0)
    gathered(1)

    def beside_second(k):
        @pl.when(k < groups)
        def _():
            pass_on(0, k)

        @pl.when((k >= groups) & (k < 2 * groups))
        def _():
            add_up(0, k - groups, False)

    gate_up(1, beside_second)
    sent(0)
    y_store(0).start()
    down(1)
    _each(groups - LAG, groups, lambda g: pass_on(1, g))
    _each(0, groups, lambda g: add_up(1, g, False))
    y_store(1).start()
    sent(1)
    for p in range(2):
        for c in own_copies(p) + forwards(p):
            c.wait_send()
        y_store(p).wait()


def tail(n, seen, x, gains, wo, wg, wu, wd):
    rows, d = x.shape
    p_rows = rows // 2
    groups, ff = d // GROUP, wd.shape[0]
    dma = pltpu.SemaphoreType.DMA
    hbm = pl.BlockSpec(memory_space=pl.ANY)
    return pl.pallas_call(
        functools.partial(_tail_kernel, n),
        in_specs=[hbm, hbm, pl.BlockSpec(memory_space=pltpu.VMEM), hbm, hbm, hbm, hbm],
        out_specs=hbm,
        out_shape=jax.ShapeDtypeStruct(x.shape, BF16),
        scratch_shapes=[
            pltpu.VMEM((n * p_rows, ff), BF16),
            pltpu.VMEM((2, n * p_rows, d), BF16),
            pltpu.VMEM((2, p_rows, d), BF16),
            pltpu.VMEM((2, d, TILE), BF16),
            pltpu.VMEM((2, groups, p_rows, GROUP), BF16),
            pltpu.VMEM((2, 2, groups, p_rows, GROUP), BF16),
            pltpu.VMEM((groups, p_rows, GROUP), F32),
            pltpu.VMEM((groups, 2 * p_rows, GROUP), F32),
            pltpu.VMEM((groups, p_rows, GROUP), BF16),
            pltpu.VMEM((groups, 2, p_rows, GROUP), BF16),
            pltpu.VMEM((p_rows, 128), F32),
            pltpu.VMEM((2, n * p_rows, TILE), F32),
            dma((2, n)), dma((2,)), dma((2, 2)), dma((groups, 2)), dma((groups, 2)), dma((2, groups, 2)), dma((2, groups, 2)),
            dma((2, 3, 2)), dma((2, 3, 2)),
        ],
        compiler_params=pltpu.CompilerParams(collective_id=0, has_side_effects=True, vmem_limit_bytes=67043328),
        cost_estimate=pl.CostEstimate(flops=2 * n * rows * d * (wo.shape[0] + 3 * ff), transcendentals=n * rows * ff,
                                      bytes_accessed=2 * d * (wo.shape[0] + 6 * ff)),
    )(seen, x, gains, wo, wg, wu, wd)


def solution(mesh):
    n = mesh.shape["tp"]

    def step(x, gain_a, wq, wk, wv, wo, gain_m, w_gate, w_up, w_down):
        gains = jnp.stack([gain_a, gain_m]).astype(F32)
        return tail(n, head(n, x, gains, wq, wk, wv), x, gains, wo, w_gate, w_up, w_down)

    tokens, columns, rows_of = P(("dp", "tp"), None), P(None, "tp"), P("tp", None)
    return jax.shard_map(
        step,
        mesh=mesh,
        in_specs=(tokens, P(None), columns, columns, columns, rows_of, P(None), columns, columns, rows_of),
        out_specs=tokens,
        check_vma=False,
    )
```
